256 devices in a mesh: ctx: 64 (over z, x, core), heads: 4 (over y).
Axes of the slice: x: 4, y: 4, z: 8, core: 2. Of those that a mesh axis runs over, the one named last changes fastest.
Arguments:
- query_rows: bfloat16 [64, 16, 2, 128], P('ctx', 'heads'), may hold values from -6 to 6
- past_keys: bfloat16 [64, 16, 4096, 128], P(None, 'heads', 'ctx'), may hold values from -6 to 6
- past_values: bfloat16 [64, 16, 4096, 128], P(None, 'heads', 'ctx'), may hold values from -6 to 6
- used_length: int32 [64], replicated, may hold values from 2048 to 4096
Outputs:
- read: bfloat16 [64, 16, 2, 128], P('ctx', 'heads')
The draws below stay inside these ranges and needn't reach their ends.
All inputs are finite; a program needn't handle non-finite values.
Results may differ from the reference program's by a relative error of at most 0.0015.
Values may be sent and summed in bfloat16 or wider, within the bound.
A program may use at most 64 MiB of HBM per device.

```python
import jax
import jax.numpy as jnp
from jax import lax

BATCH = 64
LENGTH = 4096
KV_HEADS = 16
GROUP = 2
HEAD_SIZE = 128


def set_ends(result, key, least, largest):
    place = [jax.random.randint(jax.random.fold_in(key, axis), (), 0, length) for axis, length in enumerate(result.shape)]
    main_axis = result.shape.index(max(result.shape))
    beside = place[:main_axis] + [(place[main_axis] + 1) % result.shape[main_axis]] + place[main_axis + 1:]
    return result.at[tuple(place)].set(least).at[tuple(beside)].set(largest)


def shard_levels(stream_key, extent, pieces, least, largest):
    def one(position, shards_of):
        draws = jax.random.uniform(jax.random.fold_in(jax.random.fold_in(stream_key, 6), position), (shards_of,), jnp.float32, least / len(pieces), largest / len(pieces))
        return jnp.repeat(jnp.exp(draws), extent[position] // shards_of).reshape((-1,) + (1,) * (len(extent) - position - 1))

    factor_of = one(*pieces[0])
    for cut in pieces[1:]:
        factor_of = factor_of * one(*cut)
    return factor_of


def gaussian(rng, shape, width, most, cuts=(), kind=jnp.bfloat16):
    drawn = width * jax.random.normal(rng, shape, jnp.float32)
    if cuts:
        drawn = drawn * shard_levels(rng, shape, cuts, -0.22, 0.18)
    return jnp.clip(drawn, -most, most).astype(kind)


def setup_inputs(seed: int = 0) -> dict:
    key_of = jax.random.split(jax.random.key(seed), 5)
    query_rows = gaussian(key_of[0], (BATCH, KV_HEADS, GROUP, HEAD_SIZE), 1.0, 6.0, ((0, 64), (1, 4)))
    past_keys = gaussian(key_of[1], (BATCH, KV_HEADS, LENGTH, HEAD_SIZE), 1.0, 6.0, ((1, 4), (2, 64)))
    past_values = gaussian(key_of[2], (BATCH, KV_HEADS, LENGTH, HEAD_SIZE), 1.0, 6.0, ((1, 4), (2, 64)))
    used_length = set_ends(jax.random.randint(key_of[3], (BATCH,), LENGTH // 2, LENGTH + 1), jax.random.fold_in(key_of[3], 1), LENGTH // 2, LENGTH).astype(jnp.int32)
    return dict(query_rows=query_rows, past_keys=past_keys, past_values=past_values, used_length=used_length)


def reference(query_rows, past_keys, past_values, used_length):
    def one_sequence(item):
        query_one, keys_one, values_one, length_one = item
        logit = jnp.einsum("kgd,ktd->kgt", query_one.astype(jnp.float32), keys_one.astype(jnp.float32)) * HEAD_SIZE ** -0.5
        logit = jnp.where(jnp.arange(LENGTH) < length_one, logit, -1e30)
        share = jax.nn.softmax(logit, axis=-1)
        return jnp.einsum("kgt,ktd->kgd", share, values_one.astype(jnp.float32), precision=lax.Precision.HIGHEST)
    read = lax.map(one_sequence, (query_rows, past_keys, past_values, used_length)).astype(jnp.bfloat16)
    return read
```

```python
import functools

import jax
import jax.numpy as jnp
from jax import lax
from jax.experimental import pallas as pl
from jax.experimental.pallas import tpu as pltpu
from jax.sharding import PartitionSpec as P

HEAD_SIZE = 128
SCALE = HEAD_SIZE ** (-0.5)
NZ, NX, NC = 8, 4, 2
NW = NX * NC
NEG = -1e30
MESH = pl.DeviceIdType.MESH
F32, BF16 = jnp.float32, jnp.bfloat16


def kernel(
    q_ref, len_ref, k_ref, v_ref, o_ref,
    kbuf, vbuf, qbuf, r1s, r1r, r2s, r2r,
    ksem, vsem, q1s_sem, q1r_sem, q2s_sem, q2r_sem, r1s_sem, r1r_sem, r2s_sem, r2r_sem,
):
    me = lax.axis_index("ctx")
    z, w = me // NW, me % NW
    x, core = w // NC, w % NC

    def z_peer(dz):
        zz = lax.rem(z + dz, NZ)
        return zz, {"ctx": zz * NW + w}

    def w_at(dx, dc):
        return lax.rem(x + dx, NX) * NC + lax.rem(core + dc, NC)

    barrier = pltpu.get_barrier_semaphore()
    for dz in range(1, NZ):
        pl.semaphore_signal(barrier, inc=1, device_id=z_peer(dz)[1], device_id_type=MESH)
    for dx in range(NX):
        for dc in range(NC):
            if dx or dc:
                pl.semaphore_signal(
                    barrier, inc=1, device_id={"ctx": z * NW + w_at(dx, dc)}, device_id_type=MESH
                )

    loads = []
    for i in range(NZ):
        rows = pl.ds(i * NW, NW)
        loads.append(pltpu.make_async_copy(k_ref.at[rows], kbuf.at[rows], ksem.at[i]))
    for i in range(NZ):
        rows = pl.ds(i * NW, NW)
        loads.append(pltpu.make_async_copy(v_ref.at[rows], vbuf.at[rows], vsem.at[i]))
    for load in loads:
        load.start()
    qbuf[w, z] = q_ref[...]

    pl.semaphore_wait(barrier, NZ - 1 + NW - 1)

    sends = []

    def send(src, dst, s_sem, r_sem, ctx):
        copy = pltpu.make_async_remote_copy(
            src_ref=src, dst_ref=dst, send_sem=s_sem, recv_sem=r_sem,
            device_id={"ctx": ctx}, device_id_type=MESH,
        )
        copy.start()
        sends.append(copy)

    def arrived(ref, sem):
        pltpu.make_async_copy(ref, ref, sem).wait()

    far_z = (4, 3, 5, 2, 6, 1, 7)
    for dz in far_z:
        zz, _ = z_peer(dz)
        send(q_ref, qbuf.at[w, z], q1s_sem.at[dz], q1r_sem.at[z], zz * NW + w)
    for dz in far_z[::-1]:
        zz, _ = z_peer(dz)
        arrived(qbuf.at[w, zz], q1r_sem.at[zz])
    far_w = ((2, 0), (2, 1), (1, 0), (3, 0), (1, 1), (3, 1), (0, 1))
    for dx, dc in far_w:
        ww = w_at(dx, dc)
        send(qbuf.at[w], qbuf.at[w], q2s_sem.at[dx * NC + dc], q2r_sem.at[w], z * NW + ww)

    base = me * 64
    lane = lax.broadcasted_iota(jnp.int32, (64, 128), 1)
    row = lax.broadcasted_iota(jnp.int32, (128, 128), 0)
    row_head = (row // 2) % 4
    lane_t = lax.broadcasted_iota(jnp.int32, (8, 128), 1) % 64 + base
    lane8 = lax.broadcasted_iota(jnp.int32, (8, 128), 1)
    row2 = lax.broadcasted_iota(jnp.int32, (8, 256), 0)
    lane2 = lax.broadcasted_iota(jnp.int32, (8, 256), 1)
    own_head = (row2 // 2) == (lane2 // 64)

    for step, dx in enumerate((0, 1, 3, 2)):
        xx = lax.rem(x + dx, NX)
        if dx == 0:
            arrived(qbuf.at[w_at(0, 1)], q2r_sem.at[w_at(0, 1)])
            for load in loads[:NZ]:
                load.wait()
        else:
            for dc in range(NC):
                arrived(qbuf.at[w_at(dx, dc)], q2r_sem.at[w_at(dx, dc)])
        queries = jnp.concatenate(
            [qbuf[xx * NC + c].astype(F32).reshape(64, 128) for c in range(NC)], axis=0
        )
        weights = jnp.concatenate(
            [jnp.where(row_head == k, queries, 0.0).astype(BF16) for k in range(4)], axis=1
        )
        members = [(c, zz) for c in range(NC) for zz in range(NZ)]
        keys = jnp.concatenate(
            [
                jnp.concatenate([kbuf[zz * NW + xx * NC + c, k] for k in range(4)], axis=1)
                for c, zz in members
            ],
            axis=0,
        )
        wide = lax.dot_general(
            keys, weights, (((1,), (1,)), ((), ())), preferred_element_type=F32
        )
        logit_t = jnp.zeros((64, 128), F32)
        for i in range(len(members)):
            logit_t = jnp.where(lane // 8 == i, wide[i * 64 : (i + 1) * 64], logit_t)
        logit_all = jnp.concatenate([logit_t, logit_t], axis=0).T * SCALE
        if dx == 0:
            for load in loads[NZ:]:
                load.wait()
        stats = [jnp.zeros((8, 128), F32) for _ in range(NC)]
        for i, (c, zz) in enumerate(members):
            b = zz * NW + xx * NC + c
            filled = lane_t < len_ref[b]
            logit = jnp.where(filled, logit_all[i * 8 : (i + 1) * 8], NEG)
            top = jnp.max(logit, axis=1, keepdims=True)
            part = jnp.where(filled, jnp.exp(logit - top), 0.0)
            total = jnp.sum(part, axis=1, keepdims=True) * 0.5
            spread = jnp.where(own_head, jnp.concatenate([part, part], axis=1), 0.0)
            high = spread.astype(BF16).astype(F32)
            both = jnp.concatenate([high, spread - high], axis=0).astype(BF16)
            out = jnp.dot(both, vbuf[b].reshape(256, 128), preferred_element_type=F32)
            r1s[xx * NC + c, zz] = out[:8] + out[8:]
            stats[c] = jnp.where(lane8 == zz, top, jnp.where(lane8 == NZ + zz, total, stats[c]))
        for c in range(NC):
            r1s[xx * NC + c, NZ] = stats[c]
        if dx == 0:
            r1r[w] = r1s[w]
        for dc in range(NC):
            if dx or dc:
                ww = w_at(dx, dc)
                send(r1s.at[ww], r1r.at[w], r1s_sem.at[dx * NC + dc], r1r_sem.at[w], z * NW + ww)

    for dx, dc in far_w:
        ww = w_at(dx, dc)
        arrived(r1r.at[ww], r1r_sem.at[ww])
    st = [r1r[s, NZ] for s in range(NW)]
    best = functools.reduce(jnp.maximum, st)
    scales = [jnp.exp(t - best) for t in st]
    totals = sum(pltpu.roll(scales[s], NZ, 1) * st[s] for s in range(NW))
    for dz in far_z + (0,):
        zz = lax.rem(z + dz, NZ)
        pick = lane8 == zz
        acc = jnp.zeros((8, 128), F32)
        for s in range(NW):
            scale = jnp.sum(jnp.where(pick, scales[s], 0.0), axis=1, keepdims=True)
            acc += scale * r1r[s, zz]
        top = jnp.sum(jnp.where(pick, best, 0.0), axis=1, keepdims=True)
        total = jnp.sum(jnp.where(lane8 == NZ + zz, totals, 0.0), axis=1, keepdims=True)
        tail = jnp.where(lane8 < 64, top, total)
        if dz == 0:
            r2r[z, 0] = acc
            r2r[z, 1] = tail
        else:
            r2s[dz, 0] = acc
            r2s[dz, 1] = tail
            send(r2s.at[dz], r2r.at[z], r2s_sem.at[dz], r2r_sem.at[z], zz * NW + w)
    for dz in far_z[::-1]:
        zz = lax.rem(z + dz, NZ)
        arrived(r2r.at[zz], r2r_sem.at[zz])
    tops = [r2r[s, 1] for s in range(NZ)]
    best = functools.reduce(jnp.maximum, tops)
    acc = jnp.zeros((8, 128), F32)
    total = jnp.zeros((8, 1), F32)
    for s in range(NZ):
        scale = jnp.exp(tops[s][:, :1] - best[:, :1])
        acc += scale * r2r[s, 0]
        total += scale * tops[s][:, 64:65]
    o_ref[...] = (acc / total).astype(o_ref.dtype)
    for copy in sends:
        copy.wait_send()


def body(query_rows, past_keys, past_values, used_length):
    vmem, dma = pltpu.VMEM, pltpu.SemaphoreType.DMA
    out = pl.pallas_call(
        kernel,
        out_shape=jax.ShapeDtypeStruct((8, HEAD_SIZE), BF16),
        in_specs=[
            pl.BlockSpec(memory_space=pltpu.VMEM),
            pl.BlockSpec(memory_space=pltpu.SMEM),
            pl.BlockSpec(memory_space=pl.ANY),
            pl.BlockSpec(memory_space=pl.ANY),
        ],
        out_specs=pl.BlockSpec(memory_space=pltpu.VMEM),
        scratch_shapes=[
            vmem(past_keys.shape, BF16),
            vmem(past_values.shape, BF16),
            vmem((NW, NZ, 8, HEAD_SIZE), BF16),
            vmem((NW, NZ + 1, 8, HEAD_SIZE), F32),
            vmem((NW, NZ + 1, 8, HEAD_SIZE), F32),
            vmem((NZ, 2, 8, HEAD_SIZE), F32),
            vmem((NZ, 2, 8, HEAD_SIZE), F32),
            dma((NZ,)), dma((NZ,)),
            dma((NZ,)), dma((NZ,)), dma((NW,)), dma((NW,)),
            dma((NW,)), dma((NW,)), dma((NZ,)), dma((NZ,)),
        ],
        compiler_params=pltpu.CompilerParams(collective_id=0, has_side_effects=True),
    )(query_rows.reshape(8, HEAD_SIZE), used_length, past_keys, past_values)
    return out.reshape(query_rows.shape)


def solution(mesh):
    return jax.shard_map(
        body,
        mesh=mesh,
        in_specs=(
            P("ctx", "heads", None, None),
            P(None, "heads", "ctx", None),
            P(None, "heads", "ctx", None),
            P(),
        ),
        out_specs=P("ctx", "heads", None, None),
        check_vma=False,
    )
```

```python
import functools

import jax
import jax.numpy as jnp
from jax import lax
from jax.experimental import pallas as pl
from jax.experimental.pallas import tpu as pltpu
from jax.sharding import PartitionSpec as P

HEAD_SIZE = 128
SCALE = HEAD_SIZE ** (-0.5)
NZ, NX, NC = 8, 4, 2
NW = NX * NC
NEG = -1e30
MESH = pl.DeviceIdType.MESH
F32, BF16 = jnp.float32, jnp.bfloat16


def kernel(
    q_hbm, len_hbm, k_ref, v_ref, o_ref,
    q_ref, len_ref,
    kbuf, vbuf, qbuf, r1s, r1r, r2s, r2r,
    qsem, lsem, ksem, vsem, q1s_sem, q1r_sem, q2s_sem, q2r_sem, r1s_sem, r1r_sem, r2s_sem, r2r_sem,
):
    me = lax.axis_index("ctx")
    z, w = me // NW, me % NW
    x, core = w // NC, w % NC

    def z_peer(dz):
        zz = lax.rem(z + dz, NZ)
        return zz, {"ctx": zz * NW + w}

    def w_at(dx, dc):
        return lax.rem(x + dx, NX) * NC + lax.rem(core + dc, NC)

    barrier = pltpu.get_barrier_semaphore()
    for dz in range(1, NZ):
        pl.semaphore_signal(barrier, inc=1, device_id=z_peer(dz)[1], device_id_type=MESH)
    for dx in range(NX):
        for dc in range(NC):
            if dx or dc:
                pl.semaphore_signal(
                    barrier, inc=1, device_id={"ctx": z * NW + w_at(dx, dc)}, device_id_type=MESH
                )

    q_load = pltpu.make_async_copy(q_hbm, q_ref, qsem)
    len_load = pltpu.make_async_copy(len_hbm, len_ref, lsem)
    q_load.start()
    len_load.start()
    loads = []
    for i in range(NZ):
        rows = pl.ds(i * NW, NW)
        loads.append(pltpu.make_async_copy(k_ref.at[rows], kbuf.at[rows], ksem.at[i]))
    for i in range(NZ):
        rows = pl.ds(i * NW, NW)
        loads.append(pltpu.make_async_copy(v_ref.at[rows], vbuf.at[rows], vsem.at[i]))
    for load in loads:
        load.start()
    q_load.wait()
    len_load.wait()
    qbuf[w, z] = q_ref[...]

    pl.semaphore_wait(barrier, NZ - 1 + NW - 1)

    sends = []

    def send(src, dst, s_sem, r_sem, ctx):
        copy = pltpu.make_async_remote_copy(
            src_ref=src, dst_ref=dst, send_sem=s_sem, recv_sem=r_sem,
            device_id={"ctx": ctx}, device_id_type=MESH,
        )
        copy.start()
        sends.append(copy)

    def arrived(ref, sem):
        pltpu.make_async_copy(ref, ref, sem).wait()

    far_z = (4, 3, 5, 2, 6, 1, 7)
    for dz in far_z:
        zz, _ = z_peer(dz)
        send(q_ref, qbuf.at[w, z], q1s_sem.at[dz], q1r_sem.at[z], zz * NW + w)
    for dz in far_z[::-1]:
        zz, _ = z_peer(dz)
        arrived(qbuf.at[w, zz], q1r_sem.at[zz])
    far_w = ((2, 0), (2, 1), (1, 0), (3, 0), (1, 1), (3, 1), (0, 1))
    for dx, dc in far_w:
        ww = w_at(dx, dc)
        send(qbuf.at[w], qbuf.at[w], q2s_sem.at[dx * NC + dc], q2r_sem.at[w], z * NW + ww)

    base = me * 64
    lane = lax.broadcasted_iota(jnp.int32, (64, 128), 1)
    row = lax.broadcasted_iota(jnp.int32, (128, 128), 0)
    row_head = (row // 2) % 4
    lane_t = lax.broadcasted_iota(jnp.int32, (8, 128), 1) % 64 + base
    lane8 = lax.broadcasted_iota(jnp.int32, (8, 128), 1)
    row2 = lax.broadcasted_iota(jnp.int32, (8, 256), 0)
    lane2 = lax.broadcasted_iota(jnp.int32, (8, 256), 1)
    own_head = (row2 // 2) == (lane2 // 64)

    for step, dx in enumerate((0, 1, 3, 2)):
        xx = lax.rem(x + dx, NX)
        if dx == 0:
            arrived(qbuf.at[w_at(0, 1)], q2r_sem.at[w_at(0, 1)])
            for load in loads[:NZ]:
                load.wait()
        else:
            for dc in range(NC):
                arrived(qbuf.at[w_at(dx, dc)], q2r_sem.at[w_at(dx, dc)])
        queries = jnp.concatenate(
            [qbuf[xx * NC + c].astype(F32).reshape(64, 128) for c in range(NC)], axis=0
        )
        weights = jnp.concatenate(
            [jnp.where(row_head == k, queries, 0.0).astype(BF16) for k in range(4)], axis=1
        )
        members = [(c, zz) for c in range(NC) for zz in range(NZ)]
        keys = jnp.concatenate(
            [
                jnp.concatenate([kbuf[zz * NW + xx * NC + c, k] for k in range(4)], axis=1)
                for c, zz in members
            ],
            axis=0,
        )
        wide = lax.dot_general(
            keys, weights, (((1,), (1,)), ((), ())), preferred_element_type=F32
        )
        logit_t = jnp.zeros((64, 128), F32)
        for i in range(len(members)):
            logit_t = jnp.where(lane // 8 == i, wide[i * 64 : (i + 1) * 64], logit_t)
        logit_all = jnp.concatenate([logit_t, logit_t], axis=0).T * SCALE
        if dx == 0:
            for load in loads[NZ:]:
                load.wait()
        stats = [jnp.zeros((8, 128), F32) for _ in range(NC)]
        for i, (c, zz) in enumerate(members):
            b = zz * NW + xx * NC + c
            filled = lane_t < len_ref[b]
            logit = jnp.where(filled, logit_all[i * 8 : (i + 1) * 8], NEG)
            top = jnp.max(logit, axis=1, keepdims=True)
            part = jnp.where(filled, jnp.exp(logit - top), 0.0)
            total = jnp.sum(part, axis=1, keepdims=True) * 0.5
            spread = jnp.where(own_head, jnp.concatenate([part, part], axis=1), 0.0)
            high = spread.astype(BF16).astype(F32)
            both = jnp.concatenate([high, spread - high], axis=0).astype(BF16)
            out = jnp.dot(both, vbuf[b].reshape(256, 128), preferred_element_type=F32)
            r1s[xx * NC + c, zz] = out[:8] + out[8:]
            stats[c] = jnp.where(lane8 == zz, top, jnp.where(lane8 == NZ + zz, total, stats[c]))
        for c in range(NC):
            r1s[xx * NC + c, NZ] = stats[c]
        if dx == 0:
            r1r[w] = r1s[w]
        for dc in range(NC):
            if dx or dc:
                ww = w_at(dx, dc)
                send(r1s.at[ww], r1r.at[w], r1s_sem.at[dx * NC + dc], r1r_sem.at[w], z * NW + ww)

    for dx, dc in far_w:
        ww = w_at(dx, dc)
        arrived(r1r.at[ww], r1r_sem.at[ww])
    st = [r1r[s, NZ] for s in range(NW)]
    best = functools.reduce(jnp.maximum, st)
    scales = [jnp.exp(t - best) for t in st]
    totals = sum(pltpu.roll(scales[s], NZ, 1) * st[s] for s in range(NW))
    for dz in far_z + (0,):
        zz = lax.rem(z + dz, NZ)
        pick = lane8 == zz
        acc = jnp.zeros((8, 128), F32)
        for s in range(NW):
            scale = jnp.sum(jnp.where(pick, scales[s], 0.0), axis=1, keepdims=True)
            acc += scale * r1r[s, zz]
        top = jnp.sum(jnp.where(pick, best, 0.0), axis=1, keepdims=True)
        total = jnp.sum(jnp.where(lane8 == NZ + zz, totals, 0.0), axis=1, keepdims=True)
        tail = jnp.where(lane8 < 64, top, total)
        if dz == 0:
            r2r[z, 0] = acc
            r2r[z, 1] = tail
        else:
            r2s[dz, 0] = acc
            r2s[dz, 1] = tail
            send(r2s.at[dz], r2r.at[z], r2s_sem.at[dz], r2r_sem.at[z], zz * NW + w)
    for dz in far_z[::-1]:
        zz = lax.rem(z + dz, NZ)
        arrived(r2r.at[zz], r2r_sem.at[zz])
    tops = [r2r[s, 1] for s in range(NZ)]
    best = functools.reduce(jnp.maximum, tops)
    acc = jnp.zeros((8, 128), F32)
    total = jnp.zeros((8, 1), F32)
    for s in range(NZ):
        scale = jnp.exp(tops[s][:, :1] - best[:, :1])
        acc += scale * r2r[s, 0]
        total += scale * tops[s][:, 64:65]
    o_ref[...] = (acc / total).astype(o_ref.dtype)
    for copy in sends:
        copy.wait_send()


def body(query_rows, past_keys, past_values, used_length):
    vmem, dma = pltpu.VMEM, pltpu.SemaphoreType.DMA
    out = pl.pallas_call(
        kernel,
        out_shape=pltpu.VMEM((8, HEAD_SIZE), BF16),
        in_specs=[
            pl.BlockSpec(memory_space=pl.ANY),
            pl.BlockSpec(memory_space=pl.ANY),
            pl.BlockSpec(memory_space=pl.ANY),
            pl.BlockSpec(memory_space=pl.ANY),
        ],
        out_specs=pl.BlockSpec(memory_space=pltpu.VMEM),
        scratch_shapes=[
            vmem((8, HEAD_SIZE), BF16),
            pltpu.SMEM((64,), jnp.int32),
            vmem(past_keys.shape, BF16),
            vmem(past_values.shape, BF16),
            vmem((NW, NZ, 8, HEAD_SIZE), BF16),
            vmem((NW, NZ + 1, 8, HEAD_SIZE), F32),
            vmem((NW, NZ + 1, 8, HEAD_SIZE), F32),
            vmem((NZ, 2, 8, HEAD_SIZE), F32),
            vmem((NZ, 2, 8, HEAD_SIZE), F32),
            dma, dma, dma((NZ,)), dma((NZ,)),
            dma((NZ,)), dma((NZ,)), dma((NW,)), dma((NW,)),
            dma((NW,)), dma((NW,)), dma((NZ,)), dma((NZ,)),
        ],
        compiler_params=pltpu.CompilerParams(collective_id=0, has_side_effects=True),
    )(query_rows.reshape(8, HEAD_SIZE), used_length, past_keys, past_values)
    return out.reshape(query_rows.shape)


def solution(mesh):
    return jax.shard_map(
        body,
        mesh=mesh,
        in_specs=(
            P("ctx", "heads", None, None),
            P(None, "heads", "ctx", None),
            P(None, "heads", "ctx", None),
            P(),
        ),
        out_specs=P("ctx", "heads", None, None),
        check_vma=False,
    )
```

```python
import functools

import jax
import jax.numpy as jnp
from jax import lax
from jax.experimental import pallas as pl
from jax.experimental.pallas import tpu as pltpu
from jax.sharding import PartitionSpec as P

HEAD_SIZE = 128
SCALE = HEAD_SIZE ** (-0.5)
NZ, NX, NC = 8, 4, 2
NW = NX * NC
NEG = -1e30
MESH = pl.DeviceIdType.MESH
F32, BF16 = jnp.float32, jnp.bfloat16


def kernel(
    q_hbm, len_hbm, k_ref, v_ref, o_ref,
    len_ref, kbuf, vbuf, qbuf, r1s, r1r, r2s, r2r,
    qsem, lsem, ksem, vsem, ready,
    xs_sem, xr_sem, zs_sem, zr_sem, r1s_sem, r1r_sem, r2s_sem, r2r_sem,
):
    me = lax.axis_index("ctx")
    z, w = me // NW, me % NW
    x, core = w // NC, w % NC
    late = z // 4
    pair = z // 2

    def w_at(dx, dc):
        return lax.rem(x + dx, NX) * NC + lax.rem(core + dc, NC)

    far_w = [w_at(*d) for d in ((2, 0), (2, 1), (1, 0), (3, 0), (1, 1), (3, 1), (0, 1))]
    pairs = [pair, pair + 1 - 2 * (pair % 2), 3 - pair, (pair + 2) % 4]
    planes = [2 * p + (z + a) % 2 for p in pairs for a in range(2)]
    work = [planes[i] + late * (planes[(i + 4) % NZ] - planes[i]) for i in range(NZ)]
    starts = [work[i] // 2 * 2 for i in range(0, NZ, 2)]

    barrier = pltpu.get_barrier_semaphore()

    def signal(sem, zz, ww):
        pl.semaphore_signal(sem, inc=1, device_id={"ctx": zz * NW + ww}, device_id_type=MESH)

    for ww in far_w:
        signal(barrier, z, ww)
    for zz in planes[1:4]:
        signal(barrier, zz, w)

    @pl.when(late == 0)
    def _():
        for zz in planes[4:]:
            signal(barrier, zz, w)

    q_load = pltpu.make_async_copy(q_hbm, qbuf.at[z, w], qsem)
    len_load = pltpu.make_async_copy(len_hbm, len_ref, lsem)
    q_load.start()
    len_load.start()
    loads = []
    for src, dst, sem in ((k_ref, kbuf, ksem), (v_ref, vbuf, vsem)):
        for i, start in enumerate(starts):
            rows = pl.ds(start * NW, 2 * NW)
            loads.append(pltpu.make_async_copy(src.at[rows], dst.at[rows], sem.at[i]))
    q_load.wait()
    for load in loads:
        load.start()
    pl.semaphore_wait(barrier, 10 + 4 * late)

    @pl.when(late == 1)
    def _():
        for zz in planes[4:]:
            signal(ready.at[z - 4], zz, w)

    def send(src, dst, s_sem, r_sem, zz, ww):
        copy = pltpu.make_async_remote_copy(
            src_ref=src, dst_ref=dst, send_sem=s_sem, recv_sem=r_sem,
            device_id={"ctx": zz * NW + ww}, device_id_type=MESH,
        )
        copy.start()

    def arrived(ref, sem):
        pltpu.make_async_copy(ref, ref, sem).wait()

    for ww in far_w:
        send(qbuf.at[z, w], qbuf.at[z, w], xs_sem, xr_sem, z, ww)
    arrived(qbuf.at[z, pl.ds(0, NW - 1)], xr_sem)
    for i, zz in enumerate(planes):
        if i >= 4:

            @pl.when(late == 0)
            def _():
                pl.semaphore_wait(ready.at[zz - 4], 1)

        if i:
            send(qbuf.at[z], qbuf.at[z], zs_sem, zr_sem.at[z], zz, w)

    base = me * 64
    lane = lax.broadcasted_iota(jnp.int32, (64, 128), 1)
    row = lax.broadcasted_iota(jnp.int32, (128, 128), 0)
    row_head = (row // 2) % 4
    lane8 = lax.broadcasted_iota(jnp.int32, (8, 128), 1)
    lane_t = lane8 % 64 + base
    row2 = lax.broadcasted_iota(jnp.int32, (8, 256), 0)
    lane2 = lax.broadcasted_iota(jnp.int32, (8, 256), 1)
    own_head = (row2 // 2) == (lane2 // 64)

    def attend(step):
        half, first = step // 2, 2 * (step % 2)
        mine = work[2 * step : 2 * step + 2]
        for i in range(2 * step, 2 * step + 2):
            if i % 4:
                arrived(qbuf.at[work[i]], zr_sem.at[work[i]])
            else:

                @pl.when(work[i] != z)
                def _():
                    arrived(qbuf.at[work[i]], zr_sem.at[work[i]])

        loads[step].wait()
        queries = jnp.concatenate(
            [qbuf[zz].astype(F32).reshape(64, 128) for zz in mine], axis=0
        )
        weights = jnp.concatenate(
            [jnp.where(row_head == k, queries, 0.0).astype(BF16) for k in range(4)], axis=1
        )
        members = [(a, ww) for a in range(2) for ww in range(NW)]
        keys = jnp.concatenate(
            [
                jnp.concatenate([kbuf[mine[a] * NW + ww, k] for k in range(4)], axis=1)
                for a, ww in members
            ],
            axis=0,
        )
        wide = lax.dot_general(
            keys, weights, (((1,), (1,)), ((), ())), preferred_element_type=F32
        )
        logit_t = jnp.zeros((64, 128), F32)
        for i in range(len(members)):
            logit_t = jnp.where(lane // 8 == i, wide[i * 64 : (i + 1) * 64], logit_t)
        logit_all = jnp.concatenate([logit_t, logit_t], axis=0).T * SCALE
        loads[4 + step].wait()
        if step == 0:
            len_load.wait()
        for i, (a, ww) in enumerate(members):
            b = mine[a] * NW + ww
            filled = lane_t < len_ref[b]
            logit = jnp.where(filled, logit_all[i * 8 : (i + 1) * 8], NEG)
            top = jnp.max(logit, axis=1, keepdims=True)
            part = jnp.where(filled, jnp.exp(logit - top), 0.0)
            total = jnp.sum(part, axis=1, keepdims=True) * 0.5
            spread = jnp.where(own_head, jnp.concatenate([part, part], axis=1), 0.0)
            high = spread.astype(BF16).astype(F32)
            both = jnp.concatenate([high, spread - high], axis=0).astype(BF16)
            out = jnp.dot(both, vbuf[b].reshape(256, 128), preferred_element_type=F32)
            r1s[half, ww, first + a] = out[:8] + out[8:]
            stats = r1s[half, ww, 4] if first + a else jnp.zeros((8, 128), F32)
            stats = jnp.where(lane8 == first + a, top, stats)
            r1s[half, ww, 4] = jnp.where(lane8 == 4 + first + a, total, stats)

    def reduce(half):
        arrived(r1r.at[half, pl.ds(0, NW - 1)], r1r_sem.at[half])
        st = [r1r[half, s, 4] for s in range(NW)]
        best = functools.reduce(jnp.maximum, st)
        scales = [jnp.exp(t - best) for t in st]
        totals = sum(pltpu.roll(scales[s], 4, 1) * st[s] for s in range(NW))
        for slot in (3, 2, 1, 0):
            zz = work[4 * half + slot]
            acc = jnp.zeros((8, 128), F32)
            for s in range(NW):
                acc += scales[s][:, slot : slot + 1] * r1r[half, s, slot]
            tail = jnp.where(lane8 < 64, best[:, slot : slot + 1], totals[:, 4 + slot : 5 + slot])
            i = 4 * half + slot
            r2s[i, 0] = acc
            r2s[i, 1] = tail
            if slot:
                send(r2s.at[i], r2r.at[z], r2s_sem, r2r_sem, zz, w)
            else:

                @pl.when(zz != z)
                def _():
                    send(r2s.at[i], r2r.at[z], r2s_sem, r2r_sem, zz, w)

                @pl.when(zz == z)
                def _():
                    r2r[z] = r2s[i]


    for half in range(2):
        attend(2 * half)
        attend(2 * half + 1)
        r1r[half, w] = r1s[half, w]
        for ww in far_w:
            send(r1s.at[half, ww], r1r.at[half, w], r1s_sem.at[half], r1r_sem.at[half], z, ww)
    reduce(0)
    reduce(1)
    arrived(r2r.at[pl.ds(0, NZ - 1)], r2r_sem)
    tops = [r2r[s, 1] for s in range(NZ)]
    best = functools.reduce(jnp.maximum, tops)
    acc = jnp.zeros((8, 128), F32)
    total = jnp.zeros((8, 1), F32)
    for s in range(NZ):
        scale = jnp.exp(tops[s][:, :1] - best[:, :1])
        acc += scale * r2r[s, 0]
        total += scale * tops[s][:, 64:65]
    o_ref[...] = (acc / total).astype(o_ref.dtype)
    arrived(qbuf.at[z, pl.ds(0, NW - 1)], xs_sem)
    arrived(qbuf.at[pl.ds(0, NZ - 1)], zs_sem)
    for half in range(2):
        arrived(r1s.at[half, pl.ds(0, NW - 1)], r1s_sem.at[half])
    arrived(r2s.at[pl.ds(0, NZ - 1)], r2s_sem)


def body(query_rows, past_keys, past_values, used_length):
    vmem, dma = pltpu.VMEM, pltpu.SemaphoreType.DMA
    out = pl.pallas_call(
        kernel,
        out_shape=pltpu.VMEM((8, HEAD_SIZE), BF16),
        in_specs=[pl.BlockSpec(memory_space=pl.ANY)] * 4,
        out_specs=pl.BlockSpec(memory_space=pltpu.VMEM),
        scratch_shapes=[
            pltpu.SMEM(used_length.shape, jnp.int32),
            vmem(past_keys.shape, BF16),
            vmem(past_values.shape, BF16),
            vmem((NZ, NW, 8, HEAD_SIZE), BF16),
            vmem((2, NW, 5, 8, HEAD_SIZE), F32),
            vmem((2, NW, 5, 8, HEAD_SIZE), F32),
            vmem((NZ, 2, 8, HEAD_SIZE), F32),
            vmem((NZ, 2, 8, HEAD_SIZE), F32),
            dma, dma, dma((4,)), dma((4,)), pltpu.SemaphoreType.REGULAR((4,)),
            dma, dma, dma, dma((NZ,)), dma((2,)), dma((2,)), dma, dma,
        ],
        compiler_params=pltpu.CompilerParams(collective_id=0, has_side_effects=True),
    )(query_rows.reshape(8, HEAD_SIZE), used_length, past_keys, past_values)
    return out.reshape(query_rows.shape)


def solution(mesh):
    return jax.shard_map(
        body,
        mesh=mesh,
        in_specs=(
            P("ctx", "heads", None, None),
            P(None, "heads", "ctx", None),
            P(None, "heads", "ctx", None),
            P(),
        ),
        out_specs=P("ctx", "heads", None, None),
        check_vma=False,
    )
```

```python
import functools

import jax
import jax.numpy as jnp
from jax import lax
from jax.experimental import pallas as pl
from jax.experimental.pallas import tpu as pltpu
from jax.sharding import PartitionSpec as P

HEAD_SIZE = 128
SCALE = HEAD_SIZE ** (-0.5)
NZ, NX, NC = 8, 4, 2
NW = NX * NC
NEG = -1e30
MESH = pl.DeviceIdType.MESH
F32, BF16 = jnp.float32, jnp.bfloat16


def kernel(
    q_hbm, len_hbm, k_ref, v_ref, o_ref,
    len_ref, kbuf, vbuf, qbuf, r1s, r1r, r2s, r2r,
    qsem, lsem, ksem, vsem, ready,
    xs_sem, xr_sem, zs_sem, zr_sem, r1s_sem, r1r_sem, r2s_sem, r2r_sem,
):
    me = lax.axis_index("ctx")
    z, w = me // NW, me % NW
    x, core = w // NC, w % NC
    late = z // 4
    pair = z // 2

    def w_at(dx, dc):
        return lax.rem(x + dx, NX) * NC + lax.rem(core + dc, NC)

    far_w = [w_at(*d) for d in ((2, 0), (2, 1), (1, 0), (3, 0), (1, 1), (3, 1), (0, 1))]
    pairs = [pair, pair + 1 - 2 * (pair % 2), 3 - pair, (pair + 2) % 4]
    planes = [2 * p + (z + a) % 2 for p in pairs for a in range(2)]
    work = [planes[i] + late * (planes[(i + 4) % NZ] - planes[i]) for i in range(NZ)]
    starts = [work[i] // 2 * 2 for i in range(0, NZ, 2)]

    barrier = pltpu.get_barrier_semaphore()

    def signal(sem, zz, ww):
        pl.semaphore_signal(sem, inc=1, device_id={"ctx": zz * NW + ww}, device_id_type=MESH)

    for ww in far_w:
        signal(barrier, z, ww)
    for zz in planes[1:4]:
        signal(barrier, zz, w)

    @pl.when(late == 0)
    def _():
        for zz in planes[4:]:
            signal(barrier, zz, w)

    q_load = pltpu.make_async_copy(q_hbm, qbuf.at[z, w], qsem)
    len_load = pltpu.make_async_copy(len_hbm, len_ref, lsem)
    q_load.start()
    len_load.start()
    loads = []
    for src, dst, sem in ((k_ref, kbuf, ksem), (v_ref, vbuf, vsem)):
        for i, start in enumerate(starts):
            rows = pl.ds(start * NW, 2 * NW)
            loads.append(pltpu.make_async_copy(src.at[rows], dst.at[rows], sem.at[i]))
    q_load.wait()
    for load in loads:
        load.start()
    pl.semaphore_wait(barrier, 10 + 4 * late)

    @pl.when(late == 1)
    def _():
        for zz in planes[4:]:
            signal(ready.at[z - 4], zz, w)

    def send(src, dst, s_sem, r_sem, zz, ww):
        copy = pltpu.make_async_remote_copy(
            src_ref=src, dst_ref=dst, send_sem=s_sem, recv_sem=r_sem,
            device_id={"ctx": zz * NW + ww}, device_id_type=MESH,
        )
        copy.start()

    def arrived(ref, sem):
        pltpu.make_async_copy(ref, ref, sem).wait()

    for ww in far_w:
        send(qbuf.at[z, w], qbuf.at[z, w], xs_sem, xr_sem, z, ww)
    arrived(qbuf.at[z, pl.ds(0, NW - 1)], xr_sem)
    def send_plane(zz):
        send(qbuf.at[z], qbuf.at[z], zs_sem, zr_sem.at[z], zz, w)

    for i, zz in enumerate(work):
        if i >= 4:

            @pl.when(late == 0)
            def _():
                pl.semaphore_wait(ready.at[zz - 4], 1)

        if i % 4:
            send_plane(zz)
        else:
            pl.when(zz != z)(functools.partial(send_plane, zz))

    base = me * 64
    lane = lax.broadcasted_iota(jnp.int32, (64, 128), 1)
    row = lax.broadcasted_iota(jnp.int32, (128, 128), 0)
    row_head = (row // 2) % 4
    lane8 = lax.broadcasted_iota(jnp.int32, (8, 128), 1)
    lane_t = lane8 % 64 + base
    row2 = lax.broadcasted_iota(jnp.int32, (8, 256), 0)
    lane2 = lax.broadcasted_iota(jnp.int32, (8, 256), 1)
    own_head = (row2 // 2) == (lane2 // 64)

    def attend(step):
        half, first = step // 2, 2 * (step % 2)
        mine = work[2 * step : 2 * step + 2]
        for i in range(2 * step, 2 * step + 2):
            if i % 4:
                arrived(qbuf.at[work[i]], zr_sem.at[work[i]])
            else:

                @pl.when(work[i] != z)
                def _():
                    arrived(qbuf.at[work[i]], zr_sem.at[work[i]])

        loads[step].wait()
        queries = jnp.concatenate(
            [qbuf[zz].astype(F32).reshape(64, 128) for zz in mine], axis=0
        )
        weights = jnp.concatenate(
            [jnp.where(row_head == k, queries, 0.0).astype(BF16) for k in range(4)], axis=1
        )
        members = [(a, ww) for a in range(2) for ww in range(NW)]
        keys = jnp.concatenate(
            [
                jnp.concatenate([kbuf[mine[a] * NW + ww, k] for k in range(4)], axis=1)
                for a, ww in members
            ],
            axis=0,
        )
        wide = jnp.concatenate(
            [
                lax.dot_general(
                    keys[a * 512 : (a + 1) * 512], weights, (((1,), (1,)), ((), ())),
                    preferred_element_type=F32,
                )
                for a in range(2)
            ],
            axis=0,
        )
        logit_t = jnp.zeros((64, 128), F32)
        for i in range(len(members)):
            logit_t = jnp.where(lane // 8 == i, wide[i * 64 : (i + 1) * 64], logit_t)
        logit_all = jnp.concatenate([logit_t, logit_t], axis=0).T * SCALE
        loads[4 + step].wait()
        if step == 0:
            len_load.wait()
        for i, (a, ww) in enumerate(members):
            b = mine[a] * NW + ww
            filled = lane_t < len_ref[b]
            logit = jnp.where(filled, logit_all[i * 8 : (i + 1) * 8], NEG)
            top = jnp.max(logit, axis=1, keepdims=True)
            part = jnp.where(filled, jnp.exp(logit - top), 0.0)
            total = jnp.sum(part, axis=1, keepdims=True) * 0.5
            spread = jnp.where(own_head, jnp.concatenate([part, part], axis=1), 0.0)
            high = spread.astype(BF16).astype(F32)
            both = jnp.concatenate([high, spread - high], axis=0).astype(BF16)
            out = jnp.dot(both, vbuf[b].reshape(256, 128), preferred_element_type=F32)
            r1s[half, ww, first + a] = out[:8] + out[8:]
            stats = r1s[half, ww, 4] if first + a else jnp.zeros((8, 128), F32)
            stats = jnp.where(lane8 == first + a, top, stats)
            r1s[half, ww, 4] = jnp.where(lane8 == 4 + first + a, total, stats)

    def reduce(half):
        arrived(r1r.at[half, pl.ds(0, NW - 1)], r1r_sem.at[half])
        st = [r1r[half, s, 4] for s in range(NW)]
        best = functools.reduce(jnp.maximum, st)
        scales = [jnp.exp(t - best) for t in st]
        totals = sum(pltpu.roll(scales[s], 4, 1) * st[s] for s in range(NW))
        for slot in (3, 2, 1, 0):
            zz = work[4 * half + slot]
            acc = jnp.zeros((8, 128), F32)
            for s in range(NW):
                acc += scales[s][:, slot : slot + 1] * r1r[half, s, slot]
            tail = jnp.where(lane8 < 64, best[:, slot : slot + 1], totals[:, 4 + slot : 5 + slot])
            i = 4 * half + slot
            r2s[i, 0] = acc
            r2s[i, 1] = tail
            if slot:
                send(r2s.at[i], r2r.at[z], r2s_sem, r2r_sem, zz, w)
            else:

                @pl.when(zz != z)
                def _():
                    send(r2s.at[i], r2r.at[z], r2s_sem, r2r_sem, zz, w)

                @pl.when(zz == z)
                def _():
                    r2r[z] = r2s[i]


    def share(half, first, count):
        part = pl.ds(first, count)
        for ww in far_w:
            send(
                r1s.at[half, ww, part], r1r.at[half, w, part],
                r1s_sem.at[half], r1r_sem.at[half], z, ww,
            )

    for half in range(2):
        attend(2 * half)
        share(half, 0, 2)
        attend(2 * half + 1)
        share(half, 2, 3)
        r1r[half, w] = r1s[half, w]
    reduce(0)
    reduce(1)
    arrived(r2r.at[pl.ds(0, NZ - 1)], r2r_sem)
    tops = [r2r[s, 1] for s in range(NZ)]
    best = functools.reduce(jnp.maximum, tops)
    acc = jnp.zeros((8, 128), F32)
    total = jnp.zeros((8, 1), F32)
    for s in range(NZ):
        scale = jnp.exp(tops[s][:, :1] - best[:, :1])
        acc += scale * r2r[s, 0]
        total += scale * tops[s][:, 64:65]
    o_ref[...] = (acc / total).astype(o_ref.dtype)
    arrived(qbuf.at[z, pl.ds(0, NW - 1)], xs_sem)
    arrived(qbuf.at[pl.ds(0, NZ - 1)], zs_sem)
    for half in range(2):
        arrived(r1s.at[half, pl.ds(0, NW - 1)], r1s_sem.at[half])
    arrived(r2s.at[pl.ds(0, NZ - 1)], r2s_sem)


def body(query_rows, past_keys, past_values, used_length):
    vmem, dma = pltpu.VMEM, pltpu.SemaphoreType.DMA
    out = pl.pallas_call(
        kernel,
        out_shape=pltpu.VMEM((8, HEAD_SIZE), BF16),
        in_specs=[pl.BlockSpec(memory_space=pl.ANY)] * 4,
        out_specs=pl.BlockSpec(memory_space=pltpu.VMEM),
        scratch_shapes=[
            pltpu.SMEM(used_length.shape, jnp.int32),
            vmem(past_keys.shape, BF16),
            vmem(past_values.shape, BF16),
            vmem((NZ, NW, 8, HEAD_SIZE), BF16),
            vmem((2, NW, 5, 8, HEAD_SIZE), F32),
            vmem((2, NW, 5, 8, HEAD_SIZE), F32),
            vmem((NZ, 2, 8, HEAD_SIZE), F32),
            vmem((NZ, 2, 8, HEAD_SIZE), F32),
            dma, dma, dma((4,)), dma((4,)), pltpu.SemaphoreType.REGULAR((4,)),
            dma, dma, dma, dma((NZ,)), dma((2,)), dma((2,)), dma, dma,
        ],
        compiler_params=pltpu.CompilerParams(collective_id=0, has_side_effects=True),
    )(query_rows.reshape(8, HEAD_SIZE), used_length, past_keys, past_values)
    return out.reshape(query_rows.shape)


def solution(mesh):
    return jax.shard_map(
        body,
        mesh=mesh,
        in_specs=(
            P("ctx", "heads", None, None),
            P(None, "heads", "ctx", None),
            P(None, "heads", "ctx", None),
            P(),
        ),
        out_specs=P("ctx", "heads", None, None),
        check_vma=False,
    )
```

```python
import functools

import jax
import jax.numpy as jnp
from jax import lax
from jax.experimental import pallas as pl
from jax.experimental.pallas import tpu as pltpu
from jax.sharding import PartitionSpec as P

HEAD_SIZE = 128
SCALE = HEAD_SIZE ** (-0.5)
NZ, NX, NC = 8, 4, 2
NW = NX * NC
NEG = -1e30
MESH = pl.DeviceIdType.MESH
F32, BF16 = jnp.float32, jnp.bfloat16


def kernel(
    q_hbm, len_hbm, k_ref, v_ref, o_ref,
    len_ref, kbuf, vbuf, qbuf, r1s, r1r, r2s, r2r,
    qsem, lsem, ksem, vsem, ready,
    xs_sem, xr_sem, zs_sem, zr_sem, cs_sem, cr_sem, r1s_sem, r1r_sem, r2s_sem, r2r_sem,
):
    me = lax.axis_index("ctx")
    z, w = me // NW, me % NW
    x, core = w // NC, w % NC
    late = z // 4
    pair = z // 2

    def w_at(dx, dc):
        return lax.rem(x + dx, NX) * NC + lax.rem(core + dc, NC)

    far_w = [w_at(*d) for d in ((2, 0), (2, 1), (1, 0), (3, 0), (1, 1), (3, 1), (0, 1))]
    pairs = [pair, pair + 1 - 2 * (pair % 2), 3 - pair, (pair + 2) % 4]
    planes = [2 * p + (z + a) % 2 for p in pairs for a in range(2)]
    work = [planes[i] + late * (planes[(i + 4) % NZ] - planes[i]) for i in range(NZ)]
    starts = [work[i] // 2 * 2 for i in range(0, NZ, 2)]

    barrier = pltpu.get_barrier_semaphore()

    def signal(sem, zz, ww):
        pl.semaphore_signal(sem, inc=1, device_id={"ctx": zz * NW + ww}, device_id_type=MESH)

    for ww in far_w:
        signal(barrier, z, ww)
    for zz in planes[1:4]:
        signal(barrier, zz, w)

    @pl.when(late == 0)
    def _():
        for zz in planes[4:]:
            signal(barrier, zz, w)

    q_load = pltpu.make_async_copy(q_hbm, qbuf.at[z, w], qsem)
    len_load = pltpu.make_async_copy(len_hbm, len_ref, lsem)
    q_load.start()
    len_load.start()
    loads = []
    for src, dst, sem in ((k_ref, kbuf, ksem), (v_ref, vbuf, vsem)):
        for i, start in enumerate(starts):
            rows = pl.ds(start * NW, 2 * NW)
            loads.append(pltpu.make_async_copy(src.at[rows], dst.at[rows], sem.at[i]))
    q_load.wait()
    for load in loads:
        load.start()
    pl.semaphore_wait(barrier, 10 + 4 * late)

    @pl.when(late == 1)
    def _():
        for zz in planes[4:]:
            signal(ready.at[z - 4], zz, w)

    def send(src, dst, s_sem, r_sem, zz, ww):
        copy = pltpu.make_async_remote_copy(
            src_ref=src, dst_ref=dst, send_sem=s_sem, recv_sem=r_sem,
            device_id={"ctx": zz * NW + ww}, device_id_type=MESH,
        )
        copy.start()

    def arrived(ref, sem):
        pltpu.make_async_copy(ref, ref, sem).wait()

    @pl.when(late == 1)
    def _():
        for zz in work[:4]:
            send(qbuf.at[z, w], qbuf.at[z, w], cs_sem, zr_sem.at[z], zz, w)

    for ww in far_w:
        send(qbuf.at[z, w], qbuf.at[z, w], xs_sem, xr_sem, z, ww)
    arrived(qbuf.at[z, pl.ds(0, NW - 1)], xr_sem)
    def send_plane(zz, wait=False):
        if wait:
            pl.semaphore_wait(ready.at[zz - 4], 1)
        send(qbuf.at[z], qbuf.at[z], zs_sem, zr_sem.at[z], zz, w)

    for zz in planes[1:4]:
        send_plane(zz)

    @pl.when(late == 0)
    def _():
        for zz in planes[4:]:
            send_plane(zz, True)


    base = me * 64
    lane = lax.broadcasted_iota(jnp.int32, (64, 128), 1)
    row = lax.broadcasted_iota(jnp.int32, (128, 128), 0)
    row_head = (row // 2) % 4
    lane8 = lax.broadcasted_iota(jnp.int32, (8, 128), 1)
    lane_t = lane8 % 64 + base
    row2 = lax.broadcasted_iota(jnp.int32, (8, 256), 0)
    lane2 = lax.broadcasted_iota(jnp.int32, (8, 256), 1)
    own_head = (row2 // 2) == (lane2 // 64)

    def attend(step):
        half, first = step // 2, 2 * (step % 2)
        mine = work[2 * step : 2 * step + 2]
        def planes_in():
            for i in range(2 * step, 2 * step + 2):
                if i % 4:
                    arrived(qbuf.at[work[i]], zr_sem.at[work[i]])
                else:

                    @pl.when(work[i] != z)
                    def _():
                        arrived(qbuf.at[work[i]], zr_sem.at[work[i]])

        if half:
            pl.when(late == 1)(planes_in)
            if step == 2:

                @pl.when(late == 0)
                def _():
                    arrived(qbuf.at[pl.ds(0, NZ - 1), pl.ds(0, 4)], cr_sem)

        else:
            planes_in()

        loads[step].wait()
        loads[4 + step].wait()
        if step == 0:
            len_load.wait()
        queries = jnp.concatenate(
            [qbuf[zz].astype(F32).reshape(64, 128) for zz in mine], axis=0
        )
        weights = jnp.concatenate(
            [jnp.where(row_head == k, queries, 0.0).astype(BF16) for k in range(4)], axis=1
        )
        members = [(a, ww) for a in range(2) for ww in range(NW)]
        keys = jnp.concatenate(
            [
                jnp.concatenate([kbuf[mine[a] * NW + ww, k] for k in range(4)], axis=1)
                for a, ww in members
            ],
            axis=0,
        )
        wide = jnp.concatenate(
            [
                lax.dot_general(
                    keys[a * 512 : (a + 1) * 512], weights, (((1,), (1,)), ((), ())),
                    preferred_element_type=F32,
                )
                for a in range(2)
            ],
            axis=0,
        )
        logit_t = jnp.zeros((64, 128), F32)
        for i in range(len(members)):
            logit_t = jnp.where(lane // 8 == i, wide[i * 64 : (i + 1) * 64], logit_t)
        logit_all = jnp.concatenate([logit_t, logit_t], axis=0).T * SCALE
        for i, (a, ww) in enumerate(members):
            b = mine[a] * NW + ww
            filled = lane_t < len_ref[b]
            logit = jnp.where(filled, logit_all[i * 8 : (i + 1) * 8], NEG)
            top = jnp.max(logit, axis=1, keepdims=True)
            part = jnp.where(filled, jnp.exp(logit - top), 0.0)
            total = jnp.sum(part, axis=1, keepdims=True) * 0.5
            spread = jnp.where(own_head, jnp.concatenate([part, part], axis=1), 0.0)
            high = spread.astype(BF16).astype(F32)
            both = jnp.concatenate([high, spread - high], axis=0).astype(BF16)
            out = jnp.dot(both, vbuf[b].reshape(256, 128), preferred_element_type=F32)
            r1s[half, ww, first + a] = out[:8] + out[8:]
            stats = r1s[half, ww, 4] if first + a else jnp.zeros((8, 128), F32)
            stats = jnp.where(lane8 == first + a, top, stats)
            r1s[half, ww, 4] = jnp.where(lane8 == 4 + first + a, total, stats)

    def reduce(half):
        arrived(r1r.at[half, pl.ds(0, NW - 1)], r1r_sem.at[half])
        st = [r1r[half, s, 4] for s in range(NW)]
        best = functools.reduce(jnp.maximum, st)
        scales = [jnp.exp(t - best) for t in st]
        totals = sum(pltpu.roll(scales[s], 4, 1) * st[s] for s in range(NW))
        for slot in (3, 2, 1, 0):
            zz = work[4 * half + slot]
            acc = jnp.zeros((8, 128), F32)
            for s in range(NW):
                acc += scales[s][:, slot : slot + 1] * r1r[half, s, slot]
            tail = jnp.where(lane8 < 64, best[:, slot : slot + 1], totals[:, 4 + slot : 5 + slot])
            i = 4 * half + slot
            r2s[i, 0] = acc
            r2s[i, 1] = tail
            if slot:
                send(r2s.at[i], r2r.at[z], r2s_sem, r2r_sem, zz, w)
            else:

                @pl.when(zz != z)
                def _():
                    send(r2s.at[i], r2r.at[z], r2s_sem, r2r_sem, zz, w)

                @pl.when(zz == z)
                def _():
                    r2r[z] = r2s[i]


    @pl.when(late == 0)
    def _():
        column = qbuf.at[pl.ds(4, 4), w]
        for zz in planes[4:]:
            arrived(qbuf.at[zz, w], zr_sem.at[zz])
        for ww in far_w:
            send(column, column, cs_sem, cr_sem, z, ww)

    def share(half, first, count):
        part = pl.ds(first, count)
        for ww in far_w:
            send(
                r1s.at[half, ww, part], r1r.at[half, w, part],
                r1s_sem.at[half], r1r_sem.at[half], z, ww,
            )

    attend(0)
    share(0, 0, 2)
    attend(1)
    share(0, 2, 3)
    r1r[0, w] = r1s[0, w]
    attend(2)
    pl.when(late == 0)(lambda: share(1, 0, 2))
    attend(3)
    pl.when(late == 0)(lambda: share(1, 2, 3))
    r1r[1, w] = r1s[1, w]
    reduce(0)
    pl.when(late == 1)(lambda: share(1, 0, 5))
    reduce(1)
    arrived(r2r.at[pl.ds(0, NZ - 1)], r2r_sem)
    tops = [r2r[s, 1] for s in range(NZ)]
    best = functools.reduce(jnp.maximum, tops)
    acc = jnp.zeros((8, 128), F32)
    total = jnp.zeros((8, 1), F32)
    for s in range(NZ):
        scale = jnp.exp(tops[s][:, :1] - best[:, :1])
        acc += scale * r2r[s, 0]
        total += scale * tops[s][:, 64:65]
    o_ref[...] = (acc / total).astype(o_ref.dtype)
    arrived(qbuf.at[z, pl.ds(0, NW - 1)], xs_sem)

    @pl.when(late == 0)
    def _():
        arrived(qbuf.at[pl.ds(0, NZ - 1)], zs_sem)
        arrived(qbuf.at[pl.ds(0, NZ - 1), pl.ds(0, 4)], cs_sem)

    @pl.when(late == 1)
    def _():
        arrived(qbuf.at[pl.ds(0, 3)], zs_sem)
        arrived(qbuf.at[0, pl.ds(0, 4)], cs_sem)

    for half in range(2):
        arrived(r1s.at[half, pl.ds(0, NW - 1)], r1s_sem.at[half])
    arrived(r2s.at[pl.ds(0, NZ - 1)], r2s_sem)


def body(query_rows, past_keys, past_values, used_length):
    vmem, dma = pltpu.VMEM, pltpu.SemaphoreType.DMA
    out = pl.pallas_call(
        kernel,
        out_shape=pltpu.VMEM((8, HEAD_SIZE), BF16),
        in_specs=[pl.BlockSpec(memory_space=pl.ANY)] * 4,
        out_specs=pl.BlockSpec(memory_space=pltpu.VMEM),
        scratch_shapes=[
            pltpu.SMEM(used_length.shape, jnp.int32),
            vmem(past_keys.shape, BF16),
            vmem(past_values.shape, BF16),
            vmem((NZ, NW, 8, HEAD_SIZE), BF16),
            vmem((2, NW, 5, 8, HEAD_SIZE), F32),
            vmem((2, NW, 5, 8, HEAD_SIZE), F32),
            vmem((NZ, 2, 8, HEAD_SIZE), F32),
            vmem((NZ, 2, 8, HEAD_SIZE), F32),
            dma, dma, dma((4,)), dma((4,)), pltpu.SemaphoreType.REGULAR((4,)),
            dma, dma, dma, dma((NZ,)), dma, dma, dma((2,)), dma((2,)), dma, dma,
        ],
        compiler_params=pltpu.CompilerParams(collective_id=0, has_side_effects=True),
    )(query_rows.reshape(8, HEAD_SIZE), used_length, past_keys, past_values)
    return out.reshape(query_rows.shape)


def solution(mesh):
    return jax.shard_map(
        body,
        mesh=mesh,
        in_specs=(
            P("ctx", "heads", None, None),
            P(None, "heads", "ctx", None),
            P(None, "heads", "ctx", None),
            P(),
        ),
        out_specs=P("ctx", "heads", None, None),
        check_vma=False,
    )
```

```python
import functools

import jax
import jax.numpy as jnp
from jax import lax
from jax.experimental import pallas as pl
from jax.experimental.pallas import tpu as pltpu
from jax.sharding import PartitionSpec as P

HEAD_SIZE = 128
SCALE = HEAD_SIZE ** (-0.5)
NZ, NX, NC = 8, 4, 2
NW = NX * NC
NEG = -1e30
MESH = pl.DeviceIdType.MESH
F32, BF16 = jnp.float32, jnp.bfloat16


def kernel(
    q_hbm, len_hbm, k_ref, v_ref, o_ref,
    len_ref, kbuf, vbuf, qbuf, r1s, r1r, r2s, r2r,
    qsem, lsem, ksem, vsem, ready,
    xs_sem, xr_sem, zs_sem, zr_sem, cs_sem, cr_sem, r1s_sem, r1r_sem, r2s_sem, r2r_sem,
):
    me = lax.axis_index("ctx")
    z, w = me // NW, me % NW
    x, core = w // NC, w % NC
    late = z // 4
    pair = z // 2

    def w_at(dx, dc):
        return lax.rem(x + dx, NX) * NC + lax.rem(core + dc, NC)

    far_w = [w_at(*d) for d in ((2, 0), (2, 1), (1, 0), (3, 0), (1, 1), (3, 1), (0, 1))]
    pairs = [pair, pair + 1 - 2 * (pair % 2), 3 - pair, (pair + 2) % 4]
    planes = [2 * p + (z + a) % 2 for p in pairs for a in range(2)]
    work = [planes[i] + late * (planes[(i + 4) % NZ] - planes[i]) for i in range(NZ)]
    starts = [work[i] // 2 * 2 for i in range(0, NZ, 2)]

    barrier = pltpu.get_barrier_semaphore()

    def signal(sem, zz, ww):
        pl.semaphore_signal(sem, inc=1, device_id={"ctx": zz * NW + ww}, device_id_type=MESH)

    for ww in far_w:
        signal(barrier, z, ww)
    for zz in range(NZ - 1, 0, -1):
        pl.when(zz > z)(functools.partial(signal, barrier, zz, w))

    q_load = pltpu.make_async_copy(q_hbm, qbuf.at[z, w], qsem)
    len_load = pltpu.make_async_copy(len_hbm, len_ref, lsem)
    q_load.start()
    len_load.start()
    loads = []
    for src, dst, sem in ((k_ref, kbuf, ksem), (v_ref, vbuf, vsem)):
        for i, start in enumerate(starts):
            rows = pl.ds(start * NW, 2 * NW)
            loads.append(pltpu.make_async_copy(src.at[rows], dst.at[rows], sem.at[i]))
    q_load.wait()
    for load in loads:
        load.start()
    pl.semaphore_wait(barrier, NW - 1 + z)

    for zz in range(NZ - 1):
        pl.when(zz < z)(functools.partial(signal, ready.at[z], zz, w))

    def send(src, dst, s_sem, r_sem, zz, ww):
        copy = pltpu.make_async_remote_copy(
            src_ref=src, dst_ref=dst, send_sem=s_sem, recv_sem=r_sem,
            device_id={"ctx": zz * NW + ww}, device_id_type=MESH,
        )
        copy.start()

    def arrived(ref, sem):
        pltpu.make_async_copy(ref, ref, sem).wait()

    @pl.when(late == 1)
    def _():
        for zz in work[:4]:
            send(qbuf.at[z, w], qbuf.at[z, w], cs_sem, zr_sem.at[z], zz, w)

    for ww in far_w:
        send(qbuf.at[z, w], qbuf.at[z, w], xs_sem, xr_sem, z, ww)
    arrived(qbuf.at[z, pl.ds(0, NW - 1)], xr_sem)
    def send_plane(zz):
        @pl.when(zz > z)
        def _():
            pl.semaphore_wait(ready.at[zz], 1)

        send(qbuf.at[z], qbuf.at[z], zs_sem, zr_sem.at[z], zz, w)

    for zz in planes[1:4]:
        send_plane(zz)

    @pl.when(late == 0)
    def _():
        for zz in planes[4:]:
            send_plane(zz)


    base = me * 64
    lane = lax.broadcasted_iota(jnp.int32, (64, 128), 1)
    row = lax.broadcasted_iota(jnp.int32, (128, 128), 0)
    row_head = (row // 2) % 4
    lane8 = lax.broadcasted_iota(jnp.int32, (8, 128), 1)
    lane_t = lane8 % 64 + base
    row2 = lax.broadcasted_iota(jnp.int32, (8, 256), 0)
    lane2 = lax.broadcasted_iota(jnp.int32, (8, 256), 1)
    own_head = (row2 // 2) == (lane2 // 64)

    def attend(step):
        half, first = step // 2, 2 * (step % 2)
        mine = work[2 * step : 2 * step + 2]
        def planes_in():
            for i in range(2 * step, 2 * step + 2):
                if i % 4:
                    arrived(qbuf.at[work[i]], zr_sem.at[work[i]])
                else:

                    @pl.when(work[i] != z)
                    def _():
                        arrived(qbuf.at[work[i]], zr_sem.at[work[i]])

        if half:
            pl.when(late == 1)(planes_in)
            if step == 2:

                @pl.when(late == 0)
                def _():
                    arrived(qbuf.at[pl.ds(0, NZ - 1), pl.ds(0, 4)], cr_sem)

        else:
            planes_in()

        loads[step].wait()
        loads[4 + step].wait()
        if step == 0:
            len_load.wait()
        queries = jnp.concatenate(
            [qbuf[zz].astype(F32).reshape(64, 128) for zz in mine], axis=0
        )
        weights = jnp.concatenate(
            [jnp.where(row_head == k, queries, 0.0).astype(BF16) for k in range(4)], axis=1
        )
        members = [(a, ww) for a in range(2) for ww in range(NW)]
        keys = jnp.concatenate(
            [
                jnp.concatenate([kbuf[mine[a] * NW + ww, k] for k in range(4)], axis=1)
                for a, ww in members
            ],
            axis=0,
        )
        wide = jnp.concatenate(
            [
                lax.dot_general(
                    keys[a * 512 : (a + 1) * 512], weights, (((1,), (1,)), ((), ())),
                    preferred_element_type=F32,
                )
                for a in range(2)
            ],
            axis=0,
        )
        logit_t = jnp.zeros((64, 128), F32)
        for i in range(len(members)):
            logit_t = jnp.where(lane // 8 == i, wide[i * 64 : (i + 1) * 64], logit_t)
        logit_all = jnp.concatenate([logit_t, logit_t], axis=0).T * SCALE
        for i, (a, ww) in enumerate(members):
            b = mine[a] * NW + ww
            filled = lane_t < len_ref[b]
            logit = jnp.where(filled, logit_all[i * 8 : (i + 1) * 8], NEG)
            top = jnp.max(logit, axis=1, keepdims=True)
            part = jnp.where(filled, jnp.exp(logit - top), 0.0)
            total = jnp.sum(part, axis=1, keepdims=True) * 0.5
            spread = jnp.where(own_head, jnp.concatenate([part, part], axis=1), 0.0)
            high = spread.astype(BF16).astype(F32)
            both = jnp.concatenate([high, spread - high], axis=0).astype(BF16)
            out = jnp.dot(both, vbuf[b].reshape(256, 128), preferred_element_type=F32)
            r1s[half, ww, first + a] = out[:8] + out[8:]
            stats = r1s[half, ww, 4] if first + a else jnp.zeros((8, 128), F32)
            stats = jnp.where(lane8 == first + a, top, stats)
            r1s[half, ww, 4] = jnp.where(lane8 == 4 + first + a, total, stats)

    def reduce(half):
        arrived(r1r.at[half, pl.ds(0, NW - 1)], r1r_sem.at[half])
        st = [r1r[half, s, 4] for s in range(NW)]
        best = functools.reduce(jnp.maximum, st)
        scales = [jnp.exp(t - best) for t in st]
        totals = sum(pltpu.roll(scales[s], 4, 1) * st[s] for s in range(NW))
        for slot in (3, 2, 1, 0):
            zz = work[4 * half + slot]
            acc = jnp.zeros((8, 128), F32)
            for s in range(NW):
                acc += scales[s][:, slot : slot + 1] * r1r[half, s, slot]
            tail = jnp.where(lane8 < 64, best[:, slot : slot + 1], totals[:, 4 + slot : 5 + slot])
            i = 4 * half + slot
            r2s[i, 0] = acc
            r2s[i, 1] = tail
            if slot:
                send(r2s.at[i], r2r.at[z], r2s_sem, r2r_sem, zz, w)
            else:

                @pl.when(zz != z)
                def _():
                    send(r2s.at[i], r2r.at[z], r2s_sem, r2r_sem, zz, w)

                @pl.when(zz == z)
                def _():
                    r2r[z] = r2s[i]


    @pl.when(late == 0)
    def _():
        column = qbuf.at[pl.ds(4, 4), w]
        for zz in planes[4:]:
            arrived(qbuf.at[zz, w], zr_sem.at[zz])
        for ww in far_w:
            send(column, column, cs_sem, cr_sem, z, ww)

    def share(half, first, count):
        part = pl.ds(first, count)
        for ww in far_w:
            send(
                r1s.at[half, ww, part], r1r.at[half, w, part],
                r1s_sem.at[half], r1r_sem.at[half], z, ww,
            )

    attend(0)
    share(0, 0, 2)
    attend(1)
    share(0, 2, 3)
    r1r[0, w] = r1s[0, w]
    attend(2)
    pl.when(late == 0)(lambda: share(1, 0, 2))
    attend(3)
    pl.when(late == 0)(lambda: share(1, 2, 3))
    r1r[1, w] = r1s[1, w]
    reduce(0)
    pl.when(late == 1)(lambda: share(1, 0, 5))
    reduce(1)
    arrived(r2r.at[pl.ds(0, NZ - 1)], r2r_sem)
    tops = [r2r[s, 1] for s in range(NZ)]
    best = functools.reduce(jnp.maximum, tops)
    acc = jnp.zeros((8, 128), F32)
    total = jnp.zeros((8, 1), F32)
    for s in range(NZ):
        scale = jnp.exp(tops[s][:, :1] - best[:, :1])
        acc += scale * r2r[s, 0]
        total += scale * tops[s][:, 64:65]
    o_ref[...] = (acc / total).astype(o_ref.dtype)
    arrived(qbuf.at[z, pl.ds(0, NW - 1)], xs_sem)

    @pl.when(late == 0)
    def _():
        arrived(qbuf.at[pl.ds(0, NZ - 1)], zs_sem)
        arrived(qbuf.at[pl.ds(0, NZ - 1), pl.ds(0, 4)], cs_sem)

    @pl.when(late == 1)
    def _():
        arrived(qbuf.at[pl.ds(0, 3)], zs_sem)
        arrived(qbuf.at[0, pl.ds(0, 4)], cs_sem)

    for half in range(2):
        arrived(r1s.at[half, pl.ds(0, NW - 1)], r1s_sem.at[half])
    arrived(r2s.at[pl.ds(0, NZ - 1)], r2s_sem)


def body(query_rows, past_keys, past_values, used_length):
    vmem, dma = pltpu.VMEM, pltpu.SemaphoreType.DMA
    out = pl.pallas_call(
        kernel,
        out_shape=pltpu.VMEM((8, HEAD_SIZE), BF16),
        in_specs=[pl.BlockSpec(memory_space=pl.ANY)] * 4,
        out_specs=pl.BlockSpec(memory_space=pltpu.VMEM),
        scratch_shapes=[
            pltpu.SMEM(used_length.shape, jnp.int32),
            vmem(past_keys.shape, BF16),
            vmem(past_values.shape, BF16),
            vmem((NZ, NW, 8, HEAD_SIZE), BF16),
            vmem((2, NW, 5, 8, HEAD_SIZE), F32),
            vmem((2, NW, 5, 8, HEAD_SIZE), F32),
            vmem((NZ, 2, 8, HEAD_SIZE), F32),
            vmem((NZ, 2, 8, HEAD_SIZE), F32),
            dma, dma, dma((4,)), dma((4,)), pltpu.SemaphoreType.REGULAR((NZ,)),
            dma, dma, dma, dma((NZ,)), dma, dma, dma((2,)), dma((2,)), dma, dma,
        ],
        compiler_params=pltpu.CompilerParams(collective_id=0, has_side_effects=True),
    )(query_rows.reshape(8, HEAD_SIZE), used_length, past_keys, past_values)
    return out.reshape(query_rows.shape)


def solution(mesh):
    return jax.shard_map(
        body,
        mesh=mesh,
        in_specs=(
            P("ctx", "heads", None, None),
            P(None, "heads", "ctx", None),
            P(None, "heads", "ctx", None),
            P(),
        ),
        out_specs=P("ctx", "heads", None, None),
        check_vma=False,
    )
```

```python
import functools

import jax
import jax.numpy as jnp
from jax import lax
from jax.experimental import pallas as pl
from jax.experimental.pallas import tpu as pltpu
from jax.sharding import PartitionSpec as P

HEAD_SIZE = 128
SCALE = HEAD_SIZE ** (-0.5)
NZ, NX, NC = 8, 4, 2
NW = NX * NC
NEG = -1e30
MESH = pl.DeviceIdType.MESH
F32, BF16 = jnp.float32, jnp.bfloat16


def kernel(
    q_hbm, len_hbm, k_ref, v_ref, o_ref,
    len_ref, kbuf, vbuf, qbuf, r1s, r1r, r2s, r2r, t2s, t2r,
    qsem, lsem, ksem, vsem, ready,
    xs_sem, xr_sem, zs_sem, zr_sem, cs_sem, cr_sem, r1s_sem, r1r_sem, r2s_sem, r2r_sem, t2s_sem, t2r_sem,
):
    me = lax.axis_index("ctx")
    z, w = me // NW, me % NW
    x, core = w // NC, w % NC
    late = z // 4
    pair = z // 2

    def w_at(dx, dc):
        return lax.rem(x + dx, NX) * NC + lax.rem(core + dc, NC)

    far_w = [w_at(*d) for d in ((2, 0), (2, 1), (1, 0), (3, 0), (1, 1), (3, 1), (0, 1))]
    pairs = [pair, pair + 1 - 2 * (pair % 2), 3 - pair, (pair + 2) % 4]
    planes = [2 * p + (z + a) % 2 for p in pairs for a in range(2)]
    work = [planes[i] + late * (planes[(i + 4) % NZ] - planes[i]) for i in range(NZ)]
    starts = [work[i] // 2 * 2 for i in range(0, NZ, 2)]

    barrier = pltpu.get_barrier_semaphore()

    def signal(sem, zz, ww):
        pl.semaphore_signal(sem, inc=1, device_id={"ctx": zz * NW + ww}, device_id_type=MESH)

    for ww in far_w:
        signal(barrier, z, ww)
    for zz in planes[1:4]:
        signal(barrier, zz, w)

    @pl.when(late == 0)
    def _():
        for zz in planes[4:]:
            signal(barrier, zz, w)

    q_load = pltpu.make_async_copy(q_hbm, qbuf.at[z, w], qsem)
    len_load = pltpu.make_async_copy(len_hbm, len_ref, lsem)
    q_load.start()
    len_load.start()
    loads = []
    for src, dst, sem in ((k_ref, kbuf, ksem), (v_ref, vbuf, vsem)):
        for i, start in enumerate(starts):
            rows = pl.ds(start * NW, 2 * NW)
            loads.append(pltpu.make_async_copy(src.at[rows], dst.at[rows], sem.at[i]))
    q_load.wait()
    for load in loads:
        load.start()
    pl.semaphore_wait(barrier, 10 + 4 * late)

    @pl.when(late == 1)
    def _():
        for zz in planes[4:]:
            signal(ready.at[z - 4], zz, w)

    def send(src, dst, s_sem, r_sem, zz, ww):
        copy = pltpu.make_async_remote_copy(
            src_ref=src, dst_ref=dst, send_sem=s_sem, recv_sem=r_sem,
            device_id={"ctx": zz * NW + ww}, device_id_type=MESH,
        )
        copy.start()

    def arrived(ref, sem):
        pltpu.make_async_copy(ref, ref, sem).wait()

    @pl.when(late == 1)
    def _():
        for zz in work[:4]:
            send(qbuf.at[z, w], qbuf.at[z, w], cs_sem, zr_sem.at[z], zz, w)

    for ww in far_w:
        send(qbuf.at[z, w], qbuf.at[z, w], xs_sem, xr_sem, z, ww)
    arrived(qbuf.at[z, pl.ds(0, NW - 1)], xr_sem)
    def send_plane(zz, wait=False):
        if wait:
            pl.semaphore_wait(ready.at[zz - 4], 1)
        send(qbuf.at[z], qbuf.at[z], zs_sem, zr_sem.at[z], zz, w)

    for zz in planes[1:4]:
        send_plane(zz)

    @pl.when(late == 0)
    def _():
        for zz in planes[4:]:
            send_plane(zz, True)


    base = me * 64
    lane = lax.broadcasted_iota(jnp.int32, (64, 128), 1)
    row = lax.broadcasted_iota(jnp.int32, (128, 128), 0)
    row_head = (row // 2) % 4
    lane8 = lax.broadcasted_iota(jnp.int32, (8, 128), 1)
    lane_t = lane8 % 64 + base
    row2 = lax.broadcasted_iota(jnp.int32, (8, 256), 0)
    lane2 = lax.broadcasted_iota(jnp.int32, (8, 256), 1)
    own_head = (row2 // 2) == (lane2 // 64)

    def attend(step):
        half, first = step // 2, 2 * (step % 2)
        mine = work[2 * step : 2 * step + 2]
        def planes_in():
            for i in range(2 * step, 2 * step + 2):
                if i % 4:
                    arrived(qbuf.at[work[i]], zr_sem.at[work[i]])
                else:

                    @pl.when(work[i] != z)
                    def _():
                        arrived(qbuf.at[work[i]], zr_sem.at[work[i]])

        if half:
            pl.when(late == 1)(planes_in)
            if step == 2:

                @pl.when(late == 0)
                def _():
                    arrived(qbuf.at[pl.ds(0, NZ - 1), pl.ds(0, 4)], cr_sem)

        else:
            planes_in()

        loads[step].wait()
        loads[4 + step].wait()
        if step == 0:
            len_load.wait()
        queries = jnp.concatenate(
            [qbuf[zz].astype(F32).reshape(64, 128) for zz in mine], axis=0
        )
        weights = jnp.concatenate(
            [jnp.where(row_head == k, queries, 0.0).astype(BF16) for k in range(4)], axis=1
        )
        members = [(a, ww) for a in range(2) for ww in range(NW)]
        keys = jnp.concatenate(
            [
                jnp.concatenate([kbuf[mine[a] * NW + ww, k] for k in range(4)], axis=1)
                for a, ww in members
            ],
            axis=0,
        )
        wide = jnp.concatenate(
            [
                lax.dot_general(
                    keys[a * 512 : (a + 1) * 512], weights, (((1,), (1,)), ((), ())),
                    preferred_element_type=F32,
                )
                for a in range(2)
            ],
            axis=0,
        )
        logit_t = jnp.zeros((64, 128), F32)
        for i in range(len(members)):
            logit_t = jnp.where(lane // 8 == i, wide[i * 64 : (i + 1) * 64], logit_t)
        logit_all = jnp.concatenate([logit_t, logit_t], axis=0).T * SCALE
        for i, (a, ww) in enumerate(members):
            b = mine[a] * NW + ww
            filled = lane_t < len_ref[b]
            logit = jnp.where(filled, logit_all[i * 8 : (i + 1) * 8], NEG)
            top = jnp.max(logit, axis=1, keepdims=True)
            part = jnp.where(filled, jnp.exp(logit - top), 0.0)
            total = jnp.sum(part, axis=1, keepdims=True) * 0.5
            spread = jnp.where(own_head, jnp.concatenate([part, part], axis=1), 0.0)
            high = spread.astype(BF16).astype(F32)
            both = jnp.concatenate([high, spread - high], axis=0).astype(BF16)
            out = jnp.dot(both, vbuf[b].reshape(256, 128), preferred_element_type=F32)
            r1s[half, ww, first + a] = out[:8] + out[8:]
            stats = r1s[half, ww, 4] if first + a else jnp.zeros((8, 128), F32)
            stats = jnp.where(lane8 == first + a, top, stats)
            r1s[half, ww, 4] = jnp.where(lane8 == 4 + first + a, total, stats)

    def reduce(half):
        arrived(r1r.at[half, pl.ds(0, NW - 1)], r1r_sem.at[half])
        st = [r1r[half, s, 4] for s in range(NW)]
        best = functools.reduce(jnp.maximum, st)
        scales = [jnp.exp(t - best) for t in st]
        totals = sum(pltpu.roll(scales[s], 4, 1) * st[s] for s in range(NW))
        rows = jnp.concatenate([jnp.where(lane8 < 4, best, totals)] * 16, axis=0).T
        for slot in (3, 2, 1, 0):
            zz = work[4 * half + slot]
            acc = jnp.zeros((8, 128), F32)
            for s in range(NW):
                acc += scales[s][:, slot : slot + 1] * r1r[half, s, slot]
            i = 4 * half + slot
            r2s[i] = acc
            t2s[i] = jnp.where(lane8[:1] < 64, rows[slot : slot + 1], rows[4 + slot : 5 + slot])

            def send_sum(i=i, zz=zz):
                send(r2s.at[i], r2r.at[z], r2s_sem, r2r_sem, zz, w)
                send(t2s.at[i], t2r.at[z], t2s_sem, t2r_sem, zz, w)

            if slot:
                send_sum()
            else:
                pl.when(zz != z)(send_sum)

                @pl.when(zz == z)
                def _():
                    r2r[z] = r2s[i]
                    t2r[z] = t2s[i]


    @pl.when(late == 0)
    def _():
        column = qbuf.at[pl.ds(4, 4), w]
        for zz in planes[4:]:
            arrived(qbuf.at[zz, w], zr_sem.at[zz])
        for ww in far_w:
            send(column, column, cs_sem, cr_sem, z, ww)

    def share(half, first, count):
        part = pl.ds(first, count)
        for ww in far_w:
            send(
                r1s.at[half, ww, part], r1r.at[half, w, part],
                r1s_sem.at[half], r1r_sem.at[half], z, ww,
            )

    attend(0)
    share(0, 0, 2)
    attend(1)
    share(0, 2, 3)
    r1r[0, w] = r1s[0, w]
    attend(2)
    pl.when(late == 0)(lambda: share(1, 0, 2))
    attend(3)
    pl.when(late == 0)(lambda: share(1, 2, 3))
    r1r[1, w] = r1s[1, w]
    reduce(0)
    pl.when(late == 1)(lambda: share(1, 0, 5))
    reduce(1)
    arrived(t2r.at[pl.ds(0, NZ - 1)], t2r_sem)
    arrived(r2r.at[pl.ds(0, NZ - 1)], r2r_sem)
    tails = t2r[...].reshape(NZ, HEAD_SIZE)
    scales = jnp.exp(tails - jnp.max(tails, axis=0, keepdims=True))
    totals = jnp.sum(pltpu.roll(scales, 64, 1) * tails, axis=0, keepdims=True)
    scales = scales / pltpu.roll(jnp.broadcast_to(totals, (NZ, HEAD_SIZE)), 64, 1)
    scales = jnp.concatenate([scales] * 16, axis=0).T[:8]
    acc = jnp.zeros((8, 128), F32)
    for s in range(NZ):
        acc += scales[:, s : s + 1] * r2r[s]
    o_ref[...] = acc.astype(o_ref.dtype)
    arrived(qbuf.at[z, pl.ds(0, NW - 1)], xs_sem)

    @pl.when(late == 0)
    def _():
        arrived(qbuf.at[pl.ds(0, NZ - 1)], zs_sem)
        arrived(qbuf.at[pl.ds(0, NZ - 1), pl.ds(0, 4)], cs_sem)

    @pl.when(late == 1)
    def _():
        arrived(qbuf.at[pl.ds(0, 3)], zs_sem)
        arrived(qbuf.at[0, pl.ds(0, 4)], cs_sem)

    for half in range(2):
        arrived(r1s.at[half, pl.ds(0, NW - 1)], r1s_sem.at[half])
    arrived(r2s.at[pl.ds(0, NZ - 1)], r2s_sem)
    arrived(t2s.at[pl.ds(0, NZ - 1)], t2s_sem)


def body(query_rows, past_keys, past_values, used_length):
    vmem, dma = pltpu.VMEM, pltpu.SemaphoreType.DMA
    out = pl.pallas_call(
        kernel,
        out_shape=pltpu.VMEM((8, HEAD_SIZE), BF16),
        in_specs=[pl.BlockSpec(memory_space=pl.ANY)] * 4,
        out_specs=pl.BlockSpec(memory_space=pltpu.VMEM),
        scratch_shapes=[
            pltpu.SMEM(used_length.shape, jnp.int32),
            vmem(past_keys.shape, BF16),
            vmem(past_values.shape, BF16),
            vmem((NZ, NW, 8, HEAD_SIZE), BF16),
            vmem((2, NW, 5, 8, HEAD_SIZE), F32),
            vmem((2, NW, 5, 8, HEAD_SIZE), F32),
            vmem((NZ, 8, HEAD_SIZE), F32),
            vmem((NZ, 8, HEAD_SIZE), F32),
            vmem((NZ, 1, HEAD_SIZE), F32),
            vmem((NZ, 1, HEAD_SIZE), F32),
            dma, dma, dma((4,)), dma((4,)), pltpu.SemaphoreType.REGULAR((4,)),
            dma, dma, dma, dma((NZ,)), dma, dma, dma((2,)), dma((2,)), dma, dma, dma, dma,
        ],
        compiler_params=pltpu.CompilerParams(collective_id=0, has_side_effects=True),
    )(query_rows.reshape(8, HEAD_SIZE), used_length, past_keys, past_values)
    return out.reshape(query_rows.shape)


def solution(mesh):
    return jax.shard_map(
        body,
        mesh=mesh,
        in_specs=(
            P("ctx", "heads", None, None),
            P(None, "heads", "ctx", None),
            P(None, "heads", "ctx", None),
            P(),
        ),
        out_specs=P("ctx", "heads", None, None),
        check_vma=False,
    )
```
